128 devices in a mesh: outer: 16 (over y_lo, z, core), inner: 8 (over y_hi, x).
Axes of the slice: x: 4, y: 4 (y_hi: 2, y_lo: 2; y = y_hi * 2 + y_lo), z: 4, core: 2. Of those that a mesh axis runs over, the one named last changes fastest.
Arguments:
- sources: float32 [262144, 512], P(('outer', 'inner')), may hold values from -6 to 6
- near_field: float32 [256, 1024, 1024], P(('outer', 'inner')), may hold values from -0.1875 to 0.1875
- project_factor: float32 [262144, 128], P(('outer', 'inner')), may hold values from -0.1875 to 0.1875
- expand_factor: float32 [262144, 128], P(('outer', 'inner')), may hold values from -0.5 to 0.5
- butterfly: float32 [4, 256, 4, 128, 128], P(None, ('outer', 'inner')), may hold values from -0.25 to 0.25
Outputs:
- scattered: float32 [262144, 512], P(('outer', 'inner'))
The draws below stay inside these ranges and needn't reach their ends.
All inputs are finite; a program needn't handle non-finite values.
Results may differ from the reference program's by a relative error of at most 0.0001.
Values sent between devices are 32-bit elements; how exact they have to be, the bound alone decides.
A program may use at most 256 MiB of HBM per device.

```python
import jax
import jax.numpy as jnp
from jax import lax

LEAF = 1024
RANK = 128
RHS = 512
CLUSTERS = 256
ROWS = 262144
LEVELS = 4


def levels(own_key, extent, cuts, low, largest):
    gain = 1.0
    for axis_at, parts in cuts:
        draws = jax.random.uniform(jax.random.fold_in(jax.random.fold_in(own_key, 6), axis_at), (parts,), jnp.float32, low / len(cuts), largest / len(cuts))
        gain = gain * jnp.repeat(jnp.exp(draws), extent[axis_at] // parts).reshape((-1,) + (1,) * (len(extent) - 1 - axis_at))
    return gain


def centred(stream_key, dims, deviation, bound, shards=(), held_as=jnp.bfloat16):
    entries = jax.random.normal(stream_key, dims, jnp.float32) * deviation
    if len(shards) > 0:
        entries = levels(stream_key, dims, shards, -0.22, 0.18) * entries
    return jnp.clip(entries, min=-bound, max=bound).astype(held_as)


def setup_inputs(seed: int = 0) -> dict:
    key_list = jax.random.split(jax.random.key(seed), 6)
    sources = centred(key_list[0], (ROWS, RHS), 1.0, 6.0, ((0, 128),), jnp.float32)
    near_field = centred(key_list[1], (CLUSTERS, LEAF, LEAF), LEAF ** -0.5, 0.1875, ((0, 128),), jnp.float32)
    project_factor = centred(key_list[2], (ROWS, RANK), LEAF ** -0.5, 0.1875, ((0, 128),), jnp.float32)
    expand_factor = centred(key_list[3], (ROWS, RANK), RANK ** -0.5, 0.5, ((0, 128),), jnp.float32)
    butterfly = centred(key_list[4], (LEVELS, CLUSTERS, 4, RANK, RANK), (4 * RANK) ** -0.5, 0.25, ((1, 128),), jnp.float32)
    return dict(sources=sources, near_field=near_field, project_factor=project_factor, expand_factor=expand_factor, butterfly=butterfly)


HIGHEST = lax.Precision.HIGHEST


def near_product(pair):
    return jnp.dot(pair[0], pair[1], precision=HIGHEST, preferred_element_type=jnp.float32)


def reference(sources, near_field, project_factor, expand_factor, butterfly):
    cluster_count, leaf_rows, _ = near_field.shape
    rank_width = project_factor.shape[1]
    rhs_count = sources.shape[1]
    source_rows = sources.reshape(cluster_count, leaf_rows, rhs_count)
    coeffs = jnp.einsum("cnk,cnr->ckr", project_factor.reshape(cluster_count, leaf_rows, rank_width), source_rows, precision=HIGHEST)
    for section_index in range(LEVELS):
        low_span = 4 ** section_index
        high_span = cluster_count // (4 * low_span)
        blocks = butterfly[section_index].reshape(high_span, 4, low_span, 4, rank_width, rank_width)
        shaped = coeffs.reshape(high_span, 4, low_span, rank_width, rhs_count)
        coeffs = jnp.einsum("hjlikm,hilmr->hjlkr", blocks, shaped, precision=HIGHEST).reshape(cluster_count, rank_width, rhs_count)
    near = lax.map(near_product, (near_field, source_rows))
    far = jnp.einsum("cnk,ckr->cnr", expand_factor.reshape(cluster_count, leaf_rows, rank_width), coeffs, precision=HIGHEST)
    return (near + far).reshape(cluster_count * leaf_rows, rhs_count)
```

```python
import functools

import jax
import jax.numpy as jnp
from jax import lax
from jax.experimental import pallas as pl
from jax.experimental.pallas import tpu as pltpu
from jax.sharding import PartitionSpec as P

MESH = pl.DeviceIdType.MESH
LANES = 128
SUBS = 8
TILES = 8
X1, X2, Y2, Z1, CO, FW, Y1, Z2 = range(8)
AT_SEND, AT_L0, AT_L1, AT_SUM1, AT_FWD, AT_L2, AT_L3, AT_SUM3 = 0, 2, 4, 6, 8, 9, 11, 13
NEAR_AT = 0


def halves(value):
    high = value.astype(jnp.bfloat16)
    low = (value - high.astype(jnp.float32)).astype(jnp.bfloat16)
    return high, low


def dot(left, right):
    return jnp.dot(left, right, preferred_element_type=jnp.float32)


def product(stacked, value):
    rows = stacked.shape[0] // 2
    high, low = halves(value)
    both = dot(stacked, jnp.concatenate([high, low], 1))
    return both[:rows, :LANES] + both[:rows, LANES:] + both[rows:, :LANES]


def kernel(
    src, near, proj, expand, fly, out,
    s_v, n_v, p_v, e_v, b_v, s_hi, s_lo, p_t, e_w, l0, l1, l2, l3, w1, w3,
    xb, xr, yb, yr, zo, zs, zr, cb, czr, cor, cfr, db, dr, fo, fs, fr,
    s_sem, n_sem, p_sem, e_sem, b_sem, w_send, w_recv, send_sem, recv_sem,
):
    outer = lax.axis_index("outer")
    inner = lax.axis_index("inner")
    x_lo, x_hi, y_hi = inner % 2, inner // 2 % 2, inner // 4
    core, z_lo, z_hi, y_lo = outer % 2, outer // 2 % 2, outer // 4 % 2, outer // 8
    inner_x1 = inner + 1 - 2 * x_lo
    inner_x2 = inner + 2 - 4 * x_hi
    inner_y2 = inner + 4 - 8 * y_hi
    outer_co = outer + 1 - 2 * core
    outer_z1 = outer + 2 - 4 * z_lo
    outer_z2 = outer + 4 - 8 * z_hi
    outer_y1 = outer + 8 - 16 * y_lo
    where = {
        X1: (outer, inner_x1),
        X2: (outer, inner_x2),
        Y2: (outer, inner_y2),
        Z1: (outer_z1, inner),
        CO: (outer_co, inner),
        FW: (outer_co, inner),
        Y1: (outer_y1, inner),
        Z2: (outer_z2, inner),
    }
    buffers = {
        X1: (xb, xr), X2: (yb, yr), Y2: (zs, zr), Z1: (cb, czr),
        CO: (cb, cor), FW: (czr, cfr), Y1: (db, dr), Z2: (fs, fr),
    }

    def exchange(step, sub):
        source, target = buffers[step]
        return pltpu.make_async_remote_copy(
            src_ref=source.at[sub],
            dst_ref=target.at[sub],
            send_sem=send_sem.at[step, sub],
            recv_sem=recv_sem.at[step, sub],
            device_id=where[step],
            device_id_type=MESH,
        )

    barrier = pltpu.get_barrier_semaphore()
    for step in (X1, X2, Y2, Z1, CO, Y1, Z2):
        pl.semaphore_signal(barrier, inc=1, device_id=where[step], device_id_type=MESH)

    def load_p(node):
        return pltpu.make_async_copy(proj.at[node], p_v.at[node], p_sem.at[node])

    def load_s(panel):
        return pltpu.make_async_copy(
            src.at[:, :, pl.ds(panel * LANES, LANES)], s_v.at[panel], s_sem.at[panel]
        )

    def load_b(level):
        return pltpu.make_async_copy(fly.at[level], b_v.at[level], b_sem.at[level])

    def load_n(tile):
        return pltpu.make_async_copy(near.at[tile], n_v.at[tile], n_sem.at[tile])

    load_e = pltpu.make_async_copy(expand, e_v, e_sem.at[0])

    load_p(0).start()
    load_p(1).start()
    for panel in range(4):
        load_s(panel).start()
    load_b(0).start()

    for node in range(2):
        load_p(node).wait()
        high, low = halves(p_v[node].T)
        p_t[node, 0:LANES, :] = high
        p_t[node, LANES : 2 * LANES, :] = low

    pl.semaphore_wait(barrier, 7)
    send_w1 = pltpu.make_async_remote_copy(
        src_ref=fly.at[1, :, 1 - y_hi],
        dst_ref=w1,
        send_sem=w_send.at[0],
        recv_sem=w_recv.at[0],
        device_id=where[Y2],
        device_id_type=MESH,
    )
    send_w3 = pltpu.make_async_remote_copy(
        src_ref=fly.at[3, :, :, 1 - z_hi],
        dst_ref=w3,
        send_sem=w_send.at[1],
        recv_sem=w_recv.at[1],
        device_id=where[Z2],
        device_id_type=MESH,
    )
    send_w1.start()
    send_w3.start()

    def project(panel, _):
        load_s(panel).wait()
        for node in range(2):
            high, low = halves(s_v[panel, node])
            columns = pl.ds(pl.multiple_of(panel * LANES, LANES), LANES)
            s_hi[node, :, columns] = high
            s_lo[node, :, columns] = low
            both = dot(p_t[node], jnp.concatenate([high, low], 1))
            xb[2 * panel + node] = (
                both[:LANES, :LANES] + both[:LANES, LANES:] + both[LANES:, :LANES]
            )

        @pl.when(panel == 0)
        def _():
            exchange(X1, 0).start()
            exchange(X1, 1).start()
            for level in range(1, 4):
                load_b(level).start()
            load_n(0).start()
            load_n(1).start()

        return 0

    lax.fori_loop(0, 4, project, 0)

    load_b(0).wait()
    for node in range(2):
        for block in range(4):
            high, low = halves(b_v[0, node, (x_lo + block // 2) % 2, block % 2])
            columns = slice(block * LANES, block * LANES + LANES)
            l0[node * LANES : node * LANES + LANES, columns] = high
            l0[(2 + node) * LANES : (3 + node) * LANES, columns] = low

    def prepare_1():
        load_b(1).wait()
        send_w1.wait_recv()
        for node in range(2):
            for block in range(2):
                digit = (x_hi + block) % 2
                columns = slice(block * LANES, block * LANES + LANES)
                high, low = halves(b_v[1, node, y_hi, digit])
                l1[node, 0:128, columns] = high
                l1[node, 256:384, columns] = low
                high, low = halves(w1[node, digit])
                l1[node, 128:256, columns] = high
                l1[node, 384:512, columns] = low

    def prepare_2():
        load_b(2).wait()
        for node in range(2):
            for block in range(4):
                high, low = halves(
                    b_v[2, node, (z_lo + block // 2) % 2, (core + block) % 2]
                )
                columns = slice(block * LANES, block * LANES + LANES)
                l2[node, 0:128, columns] = high
                l2[node, 128:256, columns] = low

    def prepare_3():
        load_b(3).wait()
        send_w3.wait_recv()
        for node in range(2):
            for block in range(2):
                digit = (y_lo + block) % 2
                columns = slice(block * LANES, block * LANES + LANES)
                high, low = halves(b_v[3, node, digit, z_hi])
                l3[node, 0:128, columns] = high
                l3[node, 256:384, columns] = low
                high, low = halves(w3[node, digit])
                l3[node, 128:256, columns] = high
                l3[node, 384:512, columns] = low

    def prepare_e():
        load_e.wait()
        for node in range(2):
            high, low = halves(e_v[node])
            e_w[node, :, 0:LANES] = high
            e_w[node, :, LANES : 2 * LANES] = low

    def level_0(panel):
        first = 2 * panel
        exchange(X1, first).wait_recv()
        exchange(X1, first + 1).wait_recv()
        value = jnp.concatenate([xb[first], xb[first + 1], xr[first], xr[first + 1]], 0)
        both = product(l0[...], value)
        yb[first] = both[:LANES]
        yb[first + 1] = both[LANES:]
        exchange(X2, first).start()
        exchange(X2, first + 1).start()

    def level_1(sub):
        exchange(X2, sub).wait_recv()
        both = product(l1[sub % 2], jnp.concatenate([yb[sub], yr[sub]], 0))
        zs[sub] = both[LANES:]
        exchange(Y2, sub).start()
        zo[sub] = both[:LANES]

    def sum_1(sub):
        exchange(Y2, sub).wait_recv()
        cb[sub] = zo[sub] + zr[sub]
        exchange(Z1, sub).start()
        exchange(CO, sub).start()

    def forward(sub):
        exchange(Z1, sub).wait_recv()
        exchange(FW, sub).start()

    def level_2(sub):
        exchange(CO, sub).wait_recv()
        exchange(FW, sub).wait_recv()
        value = jnp.concatenate([cb[sub], cor[sub], czr[sub], cfr[sub]], 0)
        db[sub] = product(l2[sub % 2], value)
        exchange(Y1, sub).start()

    def level_3(sub):
        exchange(Y1, sub).wait_recv()
        both = product(l3[sub % 2], jnp.concatenate([db[sub], dr[sub]], 0))
        fs[sub] = both[LANES:]
        exchange(Z2, sub).start()
        fo[sub] = both[:LANES]

    def sum_3(sub):
        exchange(Z2, sub).wait_recv()
        high, low = halves(fo[sub] + fr[sub])
        pair = jnp.concatenate([high, low], 1)
        both = dot(e_w[sub % 2], jnp.concatenate([pair, pair], 0))
        columns = pl.ds(pl.multiple_of(sub // 2 * LANES, LANES), LANES)
        out[sub % 2, :, columns] = out[sub % 2, :, columns] + both[:, :LANES] + both[:, LANES:]

    def near_tile(tile):
        load_n(tile).wait()
        node, row = tile // 4, pl.multiple_of(tile % 4 * 256, 256)
        high, low = halves(n_v[tile])
        right = s_hi[node]
        out[node, pl.ds(row, 256), :] = (
            dot(high, right) + dot(low, right) + dot(high, s_lo[node])
        )

    def when_sub(step, start, body):
        sub = step - start

        @pl.when((sub >= 0) & (sub < SUBS))
        def _():
            body(sub)

    def iteration(step, _):
        when_sub(step, AT_SUM3, sum_3)
        when_sub(step, AT_L3, level_3)
        when_sub(step, AT_L2, level_2)
        when_sub(step, AT_FWD, forward)
        when_sub(step, AT_SUM1, sum_1)
        when_sub(step, AT_L1, level_1)

        odd = step - AT_L0 - 1

        @pl.when((odd >= 0) & (odd < SUBS) & (odd % 2 == 0))
        def _():
            level_0(odd // 2)

        sub = step - AT_SEND

        @pl.when((sub >= 2) & (sub < SUBS))
        def _():
            exchange(X1, sub).start()

        tile = step - NEAR_AT

        @pl.when((tile >= 0) & (tile < TILES - 2))
        def _():
            load_n(tile + 2).start()

        @pl.when(tile == TILES - 2)
        def _():
            load_e.start()

        when_sub(step, NEAR_AT, near_tile)
        pl.when(step == 1)(prepare_1)
        pl.when(step == 4)(prepare_2)
        pl.when(step == 6)(prepare_3)
        pl.when(step == NEAR_AT + TILES)(prepare_e)
        return 0

    lax.fori_loop(0, AT_SUM3 + SUBS, iteration, 0)

    def drain(sub, _):
        for step in range(8):
            exchange(step, sub).wait_send()
        return 0

    lax.fori_loop(0, SUBS, drain, 0)
    send_w1.wait_send()
    send_w3.wait_send()


def body(sources, near_field, project_factor, expand_factor, butterfly):
    nodes, leaf, _ = near_field.shape
    rhs = sources.shape[1]
    rank = project_factor.shape[1]
    f32, bf16 = jnp.float32, jnp.bfloat16
    block = pltpu.VMEM((SUBS, rank, LANES), f32)
    dma = pltpu.SemaphoreType.DMA
    result = pl.pallas_call(
        kernel,
        out_shape=pltpu.VMEM((nodes, leaf, rhs), f32),
        in_specs=[pl.BlockSpec(memory_space=pl.ANY)] * 5,
        out_specs=pl.BlockSpec(memory_space=pltpu.VMEM),
        scratch_shapes=[
            pltpu.VMEM((4, nodes, leaf, LANES), f32),
            pltpu.VMEM((TILES, 256, leaf), f32),
            pltpu.VMEM((nodes, leaf, rank), f32),
            pltpu.VMEM((nodes, leaf, rank), f32),
            pltpu.VMEM((4, nodes, 2, 2, rank, rank), f32),
            pltpu.VMEM((nodes, leaf, rhs), bf16),
            pltpu.VMEM((nodes, leaf, rhs), bf16),
            pltpu.VMEM((nodes, 2 * rank, leaf), bf16),
            pltpu.VMEM((nodes, leaf, 2 * rank), bf16),
            pltpu.VMEM((4 * rank, 4 * rank), bf16),
            pltpu.VMEM((nodes, 4 * rank, 2 * rank), bf16),
            pltpu.VMEM((nodes, 2 * rank, 4 * rank), bf16),
            pltpu.VMEM((nodes, 4 * rank, 2 * rank), bf16),
            pltpu.VMEM((nodes, 2, rank, rank), f32),
            pltpu.VMEM((nodes, 2, rank, rank), f32),
        ]
        + [block] * 16
        + [
            dma((4,)), dma((TILES,)), dma((2,)), dma((1,)), dma((4,)),
            dma((2,)), dma((2,)), dma((8, SUBS)), dma((8, SUBS)),
        ],
        compiler_params=pltpu.CompilerParams(
            collective_id=0, has_side_effects=True, vmem_limit_bytes=50 * 1024 * 1024
        ),
        name="butterfly",
    )(
        sources.reshape(nodes, leaf, rhs),
        near_field.reshape(TILES, 256, leaf),
        project_factor.reshape(nodes, leaf, rank),
        expand_factor.reshape(nodes, leaf, rank),
        butterfly.reshape(butterfly.shape[0], nodes, 2, 2, rank, rank),
    )
    return result.reshape(nodes * leaf, rhs)


def solution(mesh):
    in_specs = (
        P(("outer", "inner"), None),
        P(("outer", "inner"), None, None),
        P(("outer", "inner"), None),
        P(("outer", "inner"), None),
        P(None, ("outer", "inner"), None, None, None),
    )
    out_specs = P(("outer", "inner"), None)
    return jax.shard_map(body, mesh=mesh, in_specs=in_specs, out_specs=out_specs, check_vma=False)
```

```python
import functools

import jax
import jax.numpy as jnp
from jax import lax
from jax.experimental import pallas as pl
from jax.experimental.pallas import tpu as pltpu
from jax.sharding import PartitionSpec as P

MESH = pl.DeviceIdType.MESH
LANES = 128
SUBS = 8
TILES = 8
X1, X2, Y2, Z1, CO, FW, Y1, Z2 = range(8)
AT_SEND, AT_L0, AT_L1, AT_SUM1, AT_FWD, AT_L2, AT_L3, AT_SUM3 = 0, 3, 7, 10, 13, 15, 18, 22
NEAR_AT = 0
AHEAD = 6


def halves(value):
    high = value.astype(jnp.bfloat16)
    low = (value - high.astype(jnp.float32)).astype(jnp.bfloat16)
    return high, low


def dot(left, right):
    return jnp.dot(left, right, preferred_element_type=jnp.float32)


def product(stacked, value):
    rows = stacked.shape[0] // 2
    high, low = halves(value)
    both = dot(stacked, jnp.concatenate([high, low], 1))
    return both[:rows, :LANES] + both[:rows, LANES:] + both[rows:, :LANES]


def kernel(
    src, near, proj, expand, fly, out,
    s_v, n_v, p_v, e_v, b_v, s_hi, s_lo, p_t, e_w, l0, l1, l2, l3, w1, w3,
    xb, xr, yb, yr, zo, zs, zr, cb, czr, cor, cfr, db, dr, fo, fs, fr,
    s_sem, n_sem, p_sem, e_sem, b_sem, w_send, w_recv, send_sem, recv_sem,
):
    outer = lax.axis_index("outer")
    inner = lax.axis_index("inner")
    x_lo, x_hi, y_hi = inner % 2, inner // 2 % 2, inner // 4
    core, z_lo, z_hi, y_lo = outer % 2, outer // 2 % 2, outer // 4 % 2, outer // 8
    inner_x1 = inner + 1 - 2 * x_lo
    inner_x2 = inner + 2 - 4 * x_hi
    inner_y2 = inner + 4 - 8 * y_hi
    outer_co = outer + 1 - 2 * core
    outer_z1 = outer + 2 - 4 * z_lo
    outer_z2 = outer + 4 - 8 * z_hi
    outer_y1 = outer + 8 - 16 * y_lo
    where = {
        X1: (outer, inner_x1),
        X2: (outer, inner_x2),
        Y2: (outer, inner_y2),
        Z1: (outer_z1, inner),
        CO: (outer_co, inner),
        FW: (outer_co, inner),
        Y1: (outer_y1, inner),
        Z2: (outer_z2, inner),
    }
    buffers = {
        X1: (xb, xr), X2: (yb, yr), Y2: (zs, zr), Z1: (cb, czr),
        CO: (cb, cor), FW: (czr, cfr), Y1: (db, dr), Z2: (fs, fr),
    }

    def exchange(step, sub):
        source, target = buffers[step]
        return pltpu.make_async_remote_copy(
            src_ref=source.at[sub],
            dst_ref=target.at[sub],
            send_sem=send_sem.at[step, sub],
            recv_sem=recv_sem.at[step, sub],
            device_id=where[step],
            device_id_type=MESH,
        )

    barrier = pltpu.get_barrier_semaphore()
    for step in (X1, X2, Y2, Z1, CO, Y1, Z2):
        pl.semaphore_signal(barrier, inc=1, device_id=where[step], device_id_type=MESH)

    def load_p(node):
        return pltpu.make_async_copy(proj.at[node], p_v.at[node], p_sem.at[node])

    def load_s(panel):
        return pltpu.make_async_copy(
            src.at[:, :, pl.ds(panel * LANES, LANES)], s_v.at[panel], s_sem.at[panel]
        )

    def load_b(level):
        return pltpu.make_async_copy(fly.at[level], b_v.at[level], b_sem.at[level])

    def load_n(tile):
        return pltpu.make_async_copy(near.at[tile], n_v.at[tile], n_sem.at[tile])

    load_e = pltpu.make_async_copy(expand, e_v, e_sem.at[0])

    load_p(0).start()
    load_p(1).start()
    for panel in range(4):
        load_s(panel).start()
    load_b(0).start()

    pl.semaphore_wait(barrier, 7)

    def exchange_w1(node):
        return pltpu.make_async_remote_copy(
            src_ref=fly.at[1, node, 1 - y_hi],
            dst_ref=w1.at[node],
            send_sem=w_send.at[node],
            recv_sem=w_recv.at[node],
            device_id=where[Y2],
            device_id_type=MESH,
        )

    def exchange_w3(node):
        return pltpu.make_async_remote_copy(
            src_ref=fly.at[3, node, :, 1 - z_hi],
            dst_ref=w3.at[node],
            send_sem=w_send.at[2 + node],
            recv_sem=w_recv.at[2 + node],
            device_id=where[Z2],
            device_id_type=MESH,
        )

    for node in range(2):
        exchange_w1(node).start()
        exchange_w3(node).start()

    def project(sub, _):
        panel, node = sub // 2, sub % 2

        @pl.when(panel == 0)
        def _():
            load_p(node).wait()
            high, low = halves(p_v[node].T)
            p_t[node, 0:LANES, :] = high
            p_t[node, LANES : 2 * LANES, :] = low

        @pl.when(node == 0)
        def _():
            load_s(panel).wait()

        high, low = halves(s_v[panel, node])
        columns = pl.ds(pl.multiple_of(panel * LANES, LANES), LANES)
        s_hi[node, :, columns] = high
        s_lo[node, :, columns] = low
        both = dot(p_t[node], jnp.concatenate([high, low], 1))
        xb[sub] = both[:LANES, :LANES] + both[:LANES, LANES:] + both[LANES:, :LANES]

        @pl.when(sub < AHEAD)
        def _():
            exchange(X1, sub).start()

        @pl.when(sub == 1)
        def _():
            for level in range(1, 4):
                load_b(level).start()
            load_n(0).start()
            load_n(1).start()

        return 0

    lax.fori_loop(0, SUBS, project, 0)

    load_b(0).wait()
    for node in range(2):
        for block in range(4):
            high, low = halves(b_v[0, node, (x_lo + block // 2) % 2, block % 2])
            columns = slice(block * LANES, block * LANES + LANES)
            l0[node * LANES : node * LANES + LANES, columns] = high
            l0[(2 + node) * LANES : (3 + node) * LANES, columns] = low

    def prepare_1():
        load_b(1).wait()
        for node in range(2):
            for block in range(2):
                digit = (x_hi + block) % 2
                columns = slice(block * LANES, block * LANES + LANES)
                high, low = halves(b_v[1, node, y_hi, digit])
                l1[node, 0:128, columns] = high
                l1[node, 256:384, columns] = low

    def receive_1():
        for node in range(2):
            exchange_w1(node).wait_recv()
            for block in range(2):
                digit = (x_hi + block) % 2
                columns = slice(block * LANES, block * LANES + LANES)
                high, low = halves(w1[node, digit])
                l1[node, 128:256, columns] = high
                l1[node, 384:512, columns] = low

    def prepare_2():
        load_b(2).wait()
        for node in range(2):
            for block in range(4):
                high, low = halves(
                    b_v[2, node, (z_lo + block // 2) % 2, (core + block) % 2]
                )
                columns = slice(block * LANES, block * LANES + LANES)
                l2[node, 0:128, columns] = high
                l2[node, 128:256, columns] = low

    def prepare_3():
        load_b(3).wait()
        for node in range(2):
            exchange_w3(node).wait_recv()
            for block in range(2):
                digit = (y_lo + block) % 2
                columns = slice(block * LANES, block * LANES + LANES)
                high, low = halves(b_v[3, node, digit, z_hi])
                l3[node, 0:128, columns] = high
                l3[node, 256:384, columns] = low
                high, low = halves(w3[node, digit])
                l3[node, 128:256, columns] = high
                l3[node, 384:512, columns] = low

    def prepare_e():
        load_e.wait()
        for node in range(2):
            high, low = halves(e_v[node])
            e_w[node, :, 0:LANES] = high
            e_w[node, :, LANES : 2 * LANES] = low

    def level_0(panel):
        first = 2 * panel
        exchange(X1, first).wait_recv()
        exchange(X1, first + 1).wait_recv()
        value = jnp.concatenate([xb[first], xb[first + 1], xr[first], xr[first + 1]], 0)
        both = product(l0[...], value)
        yb[first] = both[:LANES]
        yb[first + 1] = both[LANES:]
        exchange(X2, first).start()
        exchange(X2, first + 1).start()

    def level_1(sub):
        exchange(X2, sub).wait_recv()
        both = product(l1[sub % 2], jnp.concatenate([yb[sub], yr[sub]], 0))
        zs[sub] = both[LANES:]
        exchange(Y2, sub).start()
        zo[sub] = both[:LANES]

    def sum_1(sub):
        exchange(Y2, sub).wait_recv()
        cb[sub] = zo[sub] + zr[sub]
        exchange(Z1, sub).start()
        exchange(CO, sub).start()

    def forward(sub):
        exchange(Z1, sub).wait_recv()
        exchange(FW, sub).start()

    def level_2(sub):
        exchange(CO, sub).wait_recv()
        exchange(FW, sub).wait_recv()
        value = jnp.concatenate([cb[sub], cor[sub], czr[sub], cfr[sub]], 0)
        db[sub] = product(l2[sub % 2], value)
        exchange(Y1, sub).start()

    def level_3(sub):
        exchange(Y1, sub).wait_recv()
        both = product(l3[sub % 2], jnp.concatenate([db[sub], dr[sub]], 0))
        fs[sub] = both[LANES:]
        exchange(Z2, sub).start()
        fo[sub] = both[:LANES]

    def sum_3(sub):
        exchange(Z2, sub).wait_recv()
        high, low = halves(fo[sub] + fr[sub])
        pair = jnp.concatenate([high, low], 1)
        both = dot(e_w[sub % 2], jnp.concatenate([pair, pair], 0))
        columns = pl.ds(pl.multiple_of(sub // 2 * LANES, LANES), LANES)
        out[sub % 2, :, columns] = out[sub % 2, :, columns] + both[:, :LANES] + both[:, LANES:]

    def near_tile(part):
        tile = part // 2

        @pl.when(part % 2 == 0)
        def _():
            load_n(tile).wait()

        node, row = tile // 4, pl.multiple_of(tile % 4 * 256, 256)
        columns = pl.ds(pl.multiple_of(part % 2 * 256, 256), 256)
        high, low = halves(n_v[tile])
        right = s_hi[node, :, columns]
        out[node, pl.ds(row, 256), columns] = (
            dot(high, right) + dot(low, right) + dot(high, s_lo[node, :, columns])
        )

    def when_sub(step, start, body):
        sub = step - start

        @pl.when((sub >= 0) & (sub < SUBS))
        def _():
            body(sub)

    def iteration(step, _):
        when_sub(step, AT_SUM3, sum_3)
        when_sub(step, AT_L3, level_3)
        when_sub(step, AT_L2, level_2)
        when_sub(step, AT_FWD, forward)
        when_sub(step, AT_SUM1, sum_1)
        pl.when(step == AT_L1)(receive_1)
        when_sub(step, AT_L1, level_1)

        odd = step - AT_L0 - 1

        @pl.when((odd >= 0) & (odd < SUBS) & (odd % 2 == 0))
        def _():
            level_0(odd // 2)

        sub = step - AT_SEND

        @pl.when((sub >= AHEAD) & (sub < SUBS))
        def _():
            exchange(X1, sub).start()

        part = step - NEAR_AT

        @pl.when((part >= 0) & (part < TILES - 2))
        def _():
            load_n(part + 2).start()

        @pl.when(part == TILES - 2)
        def _():
            load_e.start()

        @pl.when((part >= 0) & (part < 2 * TILES))
        def _():
            near_tile(part)

        pl.when(step == 0)(prepare_1)
        pl.when(step == 5)(prepare_2)
        pl.when(step == 7)(prepare_3)
        pl.when(step == AT_SUM3 - 1)(prepare_e)
        return 0

    lax.fori_loop(0, AT_SUM3 + SUBS, iteration, 0)

    def drain(sub, _):
        for step in range(8):
            exchange(step, sub).wait_send()
        return 0

    lax.fori_loop(0, SUBS, drain, 0)
    for node in range(2):
        exchange_w1(node).wait_send()
        exchange_w3(node).wait_send()


def body(sources, near_field, project_factor, expand_factor, butterfly):
    nodes, leaf, _ = near_field.shape
    rhs = sources.shape[1]
    rank = project_factor.shape[1]
    f32, bf16 = jnp.float32, jnp.bfloat16
    block = pltpu.VMEM((SUBS, rank, LANES), f32)
    dma = pltpu.SemaphoreType.DMA
    result = pl.pallas_call(
        kernel,
        out_shape=pltpu.VMEM((nodes, leaf, rhs), f32),
        in_specs=[pl.BlockSpec(memory_space=pl.ANY)] * 5,
        out_specs=pl.BlockSpec(memory_space=pltpu.VMEM),
        scratch_shapes=[
            pltpu.VMEM((4, nodes, leaf, LANES), f32),
            pltpu.VMEM((TILES, 256, leaf), f32),
            pltpu.VMEM((nodes, leaf, rank), f32),
            pltpu.VMEM((nodes, leaf, rank), f32),
            pltpu.VMEM((4, nodes, 2, 2, rank, rank), f32),
            pltpu.VMEM((nodes, leaf, rhs), bf16),
            pltpu.VMEM((nodes, leaf, rhs), bf16),
            pltpu.VMEM((nodes, 2 * rank, leaf), bf16),
            pltpu.VMEM((nodes, leaf, 2 * rank), bf16),
            pltpu.VMEM((4 * rank, 4 * rank), bf16),
            pltpu.VMEM((nodes, 4 * rank, 2 * rank), bf16),
            pltpu.VMEM((nodes, 2 * rank, 4 * rank), bf16),
            pltpu.VMEM((nodes, 4 * rank, 2 * rank), bf16),
            pltpu.VMEM((nodes, 2, rank, rank), f32),
            pltpu.VMEM((nodes, 2, rank, rank), f32),
        ]
        + [block] * 16
        + [
            dma((4,)), dma((TILES,)), dma((2,)), dma((1,)), dma((4,)),
            dma((4,)), dma((4,)), dma((8, SUBS)), dma((8, SUBS)),
        ],
        compiler_params=pltpu.CompilerParams(
            collective_id=0, has_side_effects=True, vmem_limit_bytes=50 * 1024 * 1024
        ),
        name="butterfly",
    )(
        sources.reshape(nodes, leaf, rhs),
        near_field.reshape(TILES, 256, leaf),
        project_factor.reshape(nodes, leaf, rank),
        expand_factor.reshape(nodes, leaf, rank),
        butterfly.reshape(butterfly.shape[0], nodes, 2, 2, rank, rank),
    )
    return result.reshape(nodes * leaf, rhs)


def solution(mesh):
    in_specs = (
        P(("outer", "inner"), None),
        P(("outer", "inner"), None, None),
        P(("outer", "inner"), None),
        P(("outer", "inner"), None),
        P(None, ("outer", "inner"), None, None, None),
    )
    out_specs = P(("outer", "inner"), None)
    return jax.shard_map(body, mesh=mesh, in_specs=in_specs, out_specs=out_specs, check_vma=False)
```

```python
import functools

import jax
import jax.numpy as jnp
from jax import lax
from jax.experimental import pallas as pl
from jax.experimental.pallas import tpu as pltpu
from jax.sharding import PartitionSpec as P

MESH = pl.DeviceIdType.MESH
LANES = 128
SUBS = 8
TILES = 8
X1, X2, Y2, Z1, CO, FW, Y1, Z2 = range(8)
AT_SEND, AT_L0, AT_L1, AT_SUM1, AT_FWD, AT_L2, AT_L3, AT_SUM3 = 0, 3, 8, 11, 14, 16, 19, 23
NEAR_AT = 0


def halves(value):
    high = value.astype(jnp.bfloat16)
    low = (value - high.astype(jnp.float32)).astype(jnp.bfloat16)
    return high, low


def dot(left, right):
    return jnp.dot(left, right, preferred_element_type=jnp.float32)


def product(stacked, value):
    rows = stacked.shape[0] // 2
    high, low = halves(value)
    both = dot(stacked, jnp.concatenate([high, low], 1))
    return both[:rows, :LANES] + both[:rows, LANES:] + both[rows:, :LANES]


def kernel(
    src, near, proj, expand, fly, out,
    s_v, n_v, p_v, e_v, b_v, s_hi, s_lo, p_t, e_w, l0, l1, l2, l3, w1, w3,
    xb, xr, yb, yr, zo, zs, zr, cb, czr, cor, cfr, db, dr, fo, fs, fr,
    s_sem, n_sem, p_sem, e_sem, b_sem, w_send, w_recv, send_sem, recv_sem,
):
    outer = lax.axis_index("outer")
    inner = lax.axis_index("inner")
    x_lo, x_hi, y_hi = inner % 2, inner // 2 % 2, inner // 4
    core, z_lo, z_hi, y_lo = outer % 2, outer // 2 % 2, outer // 4 % 2, outer // 8
    ahead = 8 - 4 * core
    inner_x1 = inner + 1 - 2 * x_lo
    inner_x2 = inner + 2 - 4 * x_hi
    inner_y2 = inner + 4 - 8 * y_hi
    outer_co = outer + 1 - 2 * core
    outer_z1 = outer + 2 - 4 * z_lo
    outer_z2 = outer + 4 - 8 * z_hi
    outer_y1 = outer + 8 - 16 * y_lo
    where = {
        X1: (outer, inner_x1),
        X2: (outer, inner_x2),
        Y2: (outer, inner_y2),
        Z1: (outer_z1, inner),
        CO: (outer_co, inner),
        FW: (outer_co, inner),
        Y1: (outer_y1, inner),
        Z2: (outer_z2, inner),
    }
    buffers = {
        X1: (xb, xr), X2: (yb, yr), Y2: (zs, zr), Z1: (cb, czr),
        CO: (cb, cor), FW: (czr, cfr), Y1: (db, dr), Z2: (fs, fr),
    }

    def exchange(step, sub):
        source, target = buffers[step]
        return pltpu.make_async_remote_copy(
            src_ref=source.at[sub],
            dst_ref=target.at[sub],
            send_sem=send_sem.at[step, sub],
            recv_sem=recv_sem.at[step, sub],
            device_id=where[step],
            device_id_type=MESH,
        )

    barrier = pltpu.get_barrier_semaphore()
    for step in (X1, X2, Y2, Z1, CO, Y1, Z2):
        pl.semaphore_signal(barrier, inc=1, device_id=where[step], device_id_type=MESH)

    def load_p(node):
        return pltpu.make_async_copy(proj.at[node], p_v.at[node], p_sem.at[node])

    def load_s(panel):
        return pltpu.make_async_copy(
            src.at[:, :, pl.ds(panel * LANES, LANES)], s_v.at[panel], s_sem.at[panel]
        )

    def load_b(level):
        return pltpu.make_async_copy(fly.at[level], b_v.at[level], b_sem.at[level])

    def load_n(tile):
        return pltpu.make_async_copy(near.at[tile], n_v.at[tile], n_sem.at[tile])

    load_e = pltpu.make_async_copy(expand, e_v, e_sem.at[0])

    load_p(0).start()
    load_p(1).start()
    for panel in range(4):
        load_s(panel).start()
    load_b(0).start()

    pl.semaphore_wait(barrier, 7)

    def exchange_w1(node):
        return pltpu.make_async_remote_copy(
            src_ref=fly.at[1, node, 1 - y_hi],
            dst_ref=w1.at[node],
            send_sem=w_send.at[node],
            recv_sem=w_recv.at[node],
            device_id=where[Y2],
            device_id_type=MESH,
        )

    def exchange_w3(node):
        return pltpu.make_async_remote_copy(
            src_ref=fly.at[3, node, :, 1 - z_hi],
            dst_ref=w3.at[node],
            send_sem=w_send.at[2 + node],
            recv_sem=w_recv.at[2 + node],
            device_id=where[Z2],
            device_id_type=MESH,
        )

    for node in range(2):
        exchange_w1(node).start()
        exchange_w3(node).start()

    def project(sub, _):
        panel, node = sub // 2, sub % 2

        @pl.when(panel == 0)
        def _():
            load_p(node).wait()
            high, low = halves(p_v[node].T)
            p_t[node, 0:LANES, :] = high
            p_t[node, LANES : 2 * LANES, :] = low

        @pl.when(node == 0)
        def _():
            load_s(panel).wait()

        high, low = halves(s_v[panel, node])
        columns = pl.ds(pl.multiple_of(panel * LANES, LANES), LANES)
        s_hi[node, :, columns] = high
        s_lo[node, :, columns] = low
        both = dot(p_t[node], jnp.concatenate([high, low], 1))
        xb[sub] = both[:LANES, :LANES] + both[:LANES, LANES:] + both[LANES:, :LANES]

        @pl.when(sub < ahead)
        def _():
            exchange(X1, sub).start()

        @pl.when(sub == 1)
        def _():
            for level in range(1, 4):
                load_b(level).start()
            load_n(0).start()
            load_n(1).start()

        return 0

    lax.fori_loop(0, SUBS, project, 0)

    load_b(0).wait()
    for node in range(2):
        for block in range(4):
            high, low = halves(b_v[0, node, (x_lo + block // 2) % 2, block % 2])
            columns = slice(block * LANES, block * LANES + LANES)
            l0[node * LANES : node * LANES + LANES, columns] = high
            l0[(2 + node) * LANES : (3 + node) * LANES, columns] = low

    def prepare_1():
        load_b(1).wait()
        for node in range(2):
            for block in range(2):
                digit = (x_hi + block) % 2
                columns = slice(block * LANES, block * LANES + LANES)
                high, low = halves(b_v[1, node, y_hi, digit])
                l1[node, 0:128, columns] = high
                l1[node, 256:384, columns] = low

    def receive_1():
        for node in range(2):
            exchange_w1(node).wait_recv()
            for block in range(2):
                digit = (x_hi + block) % 2
                columns = slice(block * LANES, block * LANES + LANES)
                high, low = halves(w1[node, digit])
                l1[node, 128:256, columns] = high
                l1[node, 384:512, columns] = low

    def prepare_2():
        load_b(2).wait()
        for node in range(2):
            for block in range(4):
                high, low = halves(
                    b_v[2, node, (z_lo + block // 2) % 2, (core + block) % 2]
                )
                columns = slice(block * LANES, block * LANES + LANES)
                l2[node, 0:128, columns] = high
                l2[node, 128:256, columns] = low

    def prepare_3():
        load_b(3).wait()
        for node in range(2):
            exchange_w3(node).wait_recv()
            for block in range(2):
                digit = (y_lo + block) % 2
                columns = slice(block * LANES, block * LANES + LANES)
                high, low = halves(b_v[3, node, digit, z_hi])
                l3[node, 0:128, columns] = high
                l3[node, 256:384, columns] = low
                high, low = halves(w3[node, digit])
                l3[node, 128:256, columns] = high
                l3[node, 384:512, columns] = low

    def prepare_e():
        load_e.wait()
        for node in range(2):
            high, low = halves(e_v[node])
            e_w[node, :, 0:LANES] = high
            e_w[node, :, LANES : 2 * LANES] = low

    def level_0(panel):
        first = 2 * panel
        exchange(X1, first).wait_recv()
        exchange(X1, first + 1).wait_recv()
        value = jnp.concatenate([xb[first], xb[first + 1], xr[first], xr[first + 1]], 0)
        both = product(l0[...], value)
        yb[first] = both[:LANES]
        yb[first + 1] = both[LANES:]
        exchange(X2, first).start()
        exchange(X2, first + 1).start()

    def level_1(sub):
        exchange(X2, sub).wait_recv()
        both = product(l1[sub % 2], jnp.concatenate([yb[sub], yr[sub]], 0))
        zs[sub] = both[LANES:]
        exchange(Y2, sub).start()
        zo[sub] = both[:LANES]

    def sum_1(sub):
        exchange(Y2, sub).wait_recv()
        cb[sub] = zo[sub] + zr[sub]
        exchange(Z1, sub).start()
        exchange(CO, sub).start()

    def forward(sub):
        exchange(Z1, sub).wait_recv()
        exchange(FW, sub).start()

    def level_2(sub):
        exchange(CO, sub).wait_recv()
        exchange(FW, sub).wait_recv()
        value = jnp.concatenate([cb[sub], cor[sub], czr[sub], cfr[sub]], 0)
        db[sub] = product(l2[sub % 2], value)
        exchange(Y1, sub).start()

    def level_3(sub):
        exchange(Y1, sub).wait_recv()
        both = product(l3[sub % 2], jnp.concatenate([db[sub], dr[sub]], 0))
        fs[sub] = both[LANES:]
        exchange(Z2, sub).start()
        fo[sub] = both[:LANES]

    def sum_3(sub):
        exchange(Z2, sub).wait_recv()
        high, low = halves(fo[sub] + fr[sub])
        pair = jnp.concatenate([high, low], 1)
        both = dot(e_w[sub % 2], jnp.concatenate([pair, pair], 0))
        columns = pl.ds(pl.multiple_of(sub // 2 * LANES, LANES), LANES)
        out[sub % 2, :, columns] = out[sub % 2, :, columns] + both[:, :LANES] + both[:, LANES:]

    def near_tile(part):
        tile = part // 2

        @pl.when(part % 2 == 0)
        def _():
            load_n(tile).wait()

        node, row = tile // 4, pl.multiple_of(tile % 4 * 256, 256)
        columns = pl.ds(pl.multiple_of(part % 2 * 256, 256), 256)
        high, low = halves(n_v[tile])
        right = s_hi[node, :, columns]
        out[node, pl.ds(row, 256), columns] = (
            dot(high, right) + dot(low, right) + dot(high, s_lo[node, :, columns])
        )

    def when_sub(step, start, body):
        sub = step - start

        @pl.when((sub >= 0) & (sub < SUBS))
        def _():
            body(sub)

    def iteration(step, _):
        when_sub(step, AT_L3, level_3)
        when_sub(step, AT_L2, level_2)
        when_sub(step, AT_FWD, forward)
        when_sub(step, AT_SUM1, sum_1)
        pl.when(step == AT_L1)(receive_1)
        when_sub(step, AT_L1, level_1)

        odd = step - AT_L0 - 1

        @pl.when((odd >= 0) & (odd < SUBS) & (odd % 2 == 0))
        def _():
            level_0(odd // 2)
        when_sub(step, AT_SUM3, sum_3)

        sub = step - AT_SEND

        @pl.when((sub >= ahead) & (sub < SUBS))
        def _():
            exchange(X1, sub).start()

        part = step - NEAR_AT

        @pl.when((part >= 0) & (part < TILES - 2))
        def _():
            load_n(part + 2).start()

        @pl.when(part == TILES - 2)
        def _():
            load_e.start()

        @pl.when((part >= 0) & (part < 2 * TILES))
        def _():
            near_tile(part)

        pl.when(step == 0)(prepare_1)
        pl.when(step == 5)(prepare_2)
        pl.when(step == 7)(prepare_3)
        pl.when(step == AT_SUM3 - 1)(prepare_e)
        return 0

    lax.fori_loop(0, AT_SUM3 + SUBS, iteration, 0)

    def drain(sub, _):
        for step in range(8):
            exchange(step, sub).wait_send()
        return 0

    lax.fori_loop(0, SUBS, drain, 0)
    for node in range(2):
        exchange_w1(node).wait_send()
        exchange_w3(node).wait_send()


def body(sources, near_field, project_factor, expand_factor, butterfly):
    nodes, leaf, _ = near_field.shape
    rhs = sources.shape[1]
    rank = project_factor.shape[1]
    f32, bf16 = jnp.float32, jnp.bfloat16
    block = pltpu.VMEM((SUBS, rank, LANES), f32)
    dma = pltpu.SemaphoreType.DMA
    result = pl.pallas_call(
        kernel,
        out_shape=pltpu.VMEM((nodes, leaf, rhs), f32),
        in_specs=[pl.BlockSpec(memory_space=pl.ANY)] * 5,
        out_specs=pl.BlockSpec(memory_space=pltpu.VMEM),
        scratch_shapes=[
            pltpu.VMEM((4, nodes, leaf, LANES), f32),
            pltpu.VMEM((TILES, 256, leaf), f32),
            pltpu.VMEM((nodes, leaf, rank), f32),
            pltpu.VMEM((nodes, leaf, rank), f32),
            pltpu.VMEM((4, nodes, 2, 2, rank, rank), f32),
            pltpu.VMEM((nodes, leaf, rhs), bf16),
            pltpu.VMEM((nodes, leaf, rhs), bf16),
            pltpu.VMEM((nodes, 2 * rank, leaf), bf16),
            pltpu.VMEM((nodes, leaf, 2 * rank), bf16),
            pltpu.VMEM((4 * rank, 4 * rank), bf16),
            pltpu.VMEM((nodes, 4 * rank, 2 * rank), bf16),
            pltpu.VMEM((nodes, 2 * rank, 4 * rank), bf16),
            pltpu.VMEM((nodes, 4 * rank, 2 * rank), bf16),
            pltpu.VMEM((nodes, 2, rank, rank), f32),
            pltpu.VMEM((nodes, 2, rank, rank), f32),
        ]
        + [block] * 16
        + [
            dma((4,)), dma((TILES,)), dma((2,)), dma((1,)), dma((4,)),
            dma((4,)), dma((4,)), dma((8, SUBS)), dma((8, SUBS)),
        ],
        compiler_params=pltpu.CompilerParams(
            collective_id=0, has_side_effects=True, vmem_limit_bytes=50 * 1024 * 1024
        ),
        name="butterfly",
    )(
        sources.reshape(nodes, leaf, rhs),
        near_field.reshape(TILES, 256, leaf),
        project_factor.reshape(nodes, leaf, rank),
        expand_factor.reshape(nodes, leaf, rank),
        butterfly.reshape(butterfly.shape[0], nodes, 2, 2, rank, rank),
    )
    return result.reshape(nodes * leaf, rhs)


def solution(mesh):
    in_specs = (
        P(("outer", "inner"), None),
        P(("outer", "inner"), None, None),
        P(("outer", "inner"), None),
        P(("outer", "inner"), None),
        P(None, ("outer", "inner"), None, None, None),
    )
    out_specs = P(("outer", "inner"), None)
    return jax.shard_map(body, mesh=mesh, in_specs=in_specs, out_specs=out_specs, check_vma=False)
```

```python
import functools

import jax
import jax.numpy as jnp
from jax import lax
from jax.experimental import pallas as pl
from jax.experimental.pallas import tpu as pltpu
from jax.sharding import PartitionSpec as P

MESH = pl.DeviceIdType.MESH
LANES = 128
SUBS = 8
TILES = 8
X1, X2, Y2, Z1, CO, FW, Y1, Z2 = range(8)
AT_SEND, AT_L0, AT_L1, AT_SUM1, AT_FWD, AT_L2, AT_L3, AT_SUM3 = 0, 2, 7, 10, 13, 15, 18, 22
NEAR_AT = 0


def halves(value):
    high = value.astype(jnp.bfloat16)
    low = (value - high.astype(jnp.float32)).astype(jnp.bfloat16)
    return high, low


def dot(left, right):
    return jnp.dot(left, right, preferred_element_type=jnp.float32)


def product(stacked, value):
    rows = stacked.shape[0] // 2
    high, low = halves(value)
    both = dot(stacked, jnp.concatenate([high, low], 1))
    return both[:rows, :LANES] + both[:rows, LANES:] + both[rows:, :LANES]


def kernel(
    src, near, proj, expand, fly, out,
    s_v, n_v, p_v, e_v, b_v, s_hi, s_lo, p_t, e_w, l0, l1, l2, l3, w1, w3,
    xb, xr, yb, yr, zo, zs, zr, cb, czr, cor, cfr, db, dr, fo, fs, fr,
    s_sem, n_sem, p_sem, e_sem, b_sem, w_send, w_recv, send_sem, recv_sem,
):
    outer = lax.axis_index("outer")
    inner = lax.axis_index("inner")
    x_lo, x_hi, y_hi = inner % 2, inner // 2 % 2, inner // 4
    core, z_lo, z_hi, y_lo = outer % 2, outer // 2 % 2, outer // 4 % 2, outer // 8
    ahead = 8 - 4 * core
    inner_x1 = inner + 1 - 2 * x_lo
    inner_x2 = inner + 2 - 4 * x_hi
    inner_y2 = inner + 4 - 8 * y_hi
    outer_co = outer + 1 - 2 * core
    outer_z1 = outer + 2 - 4 * z_lo
    outer_z2 = outer + 4 - 8 * z_hi
    outer_y1 = outer + 8 - 16 * y_lo
    where = {
        X1: (outer, inner_x1),
        X2: (outer, inner_x2),
        Y2: (outer, inner_y2),
        Z1: (outer_z1, inner),
        CO: (outer_co, inner),
        FW: (outer_co, inner),
        Y1: (outer_y1, inner),
        Z2: (outer_z2, inner),
    }
    buffers = {
        X1: (xb, xr), X2: (yb, yr), Y2: (zs, zr), Z1: (cb, czr),
        CO: (cb, cor), FW: (czr, cfr), Y1: (db, dr), Z2: (fs, fr),
    }

    def exchange(step, sub):
        source, target = buffers[step]
        return pltpu.make_async_remote_copy(
            src_ref=source.at[sub],
            dst_ref=target.at[sub],
            send_sem=send_sem.at[step, sub],
            recv_sem=recv_sem.at[step, sub],
            device_id=where[step],
            device_id_type=MESH,
        )

    barrier = pltpu.get_barrier_semaphore()
    for step in (X1, X2, Y2, Z1, CO, Y1, Z2):
        pl.semaphore_signal(barrier, inc=1, device_id=where[step], device_id_type=MESH)

    def load_p(node):
        return pltpu.make_async_copy(proj.at[node], p_v.at[node], p_sem.at[node])

    def load_s(panel):
        return pltpu.make_async_copy(
            src.at[:, :, pl.ds(panel * LANES, LANES)], s_v.at[panel], s_sem.at[panel]
        )

    def load_b(level):
        return pltpu.make_async_copy(fly.at[level], b_v.at[level], b_sem.at[level])

    def load_n(tile):
        return pltpu.make_async_copy(near.at[tile], n_v.at[tile], n_sem.at[tile])

    load_e = pltpu.make_async_copy(expand, e_v, e_sem.at[0])

    load_p(0).start()
    load_p(1).start()
    for panel in range(4):
        load_s(panel).start()
    load_b(0).start()

    pl.semaphore_wait(barrier, 7)

    def exchange_w1(node):
        return pltpu.make_async_remote_copy(
            src_ref=fly.at[1, node, 1 - y_hi],
            dst_ref=w1.at[node],
            send_sem=w_send.at[node],
            recv_sem=w_recv.at[node],
            device_id=where[Y2],
            device_id_type=MESH,
        )

    def exchange_w3(node):
        return pltpu.make_async_remote_copy(
            src_ref=fly.at[3, node, :, 1 - z_hi],
            dst_ref=w3.at[node],
            send_sem=w_send.at[2 + node],
            recv_sem=w_recv.at[2 + node],
            device_id=where[Z2],
            device_id_type=MESH,
        )

    for node in range(2):
        exchange_w1(node).start()
        exchange_w3(node).start()

    def project(sub, _):
        panel, node = sub // 2, sub % 2

        @pl.when(panel == 0)
        def _():
            load_p(node).wait()
            high, low = halves(p_v[node].T)
            p_t[node, 0:LANES, :] = high
            p_t[node, LANES : 2 * LANES, :] = low

        @pl.when(node == 0)
        def _():
            load_s(panel).wait()

        high, low = halves(s_v[panel, node])
        columns = pl.ds(pl.multiple_of(panel * LANES, LANES), LANES)
        s_hi[node, :, columns] = high
        s_lo[node, :, columns] = low
        both = dot(p_t[node], jnp.concatenate([high, low], 1))
        xb[sub] = both[:LANES, :LANES] + both[:LANES, LANES:] + both[LANES:, :LANES]

        @pl.when(sub < ahead)
        def _():
            exchange(X1, sub).start()

        @pl.when(sub == 1)
        def _():
            for level in range(1, 4):
                load_b(level).start()
            load_n(0).start()
            load_n(1).start()

        return 0

    lax.fori_loop(0, SUBS, project, 0)

    load_b(0).wait()
    for node in range(2):
        for block in range(4):
            high, low = halves(b_v[0, node, (x_lo + block // 2) % 2, block % 2])
            columns = slice(block * LANES, block * LANES + LANES)
            l0[node * LANES : node * LANES + LANES, columns] = high
            l0[(2 + node) * LANES : (3 + node) * LANES, columns] = low

    def prepare_1():
        load_b(1).wait()
        for node in range(2):
            for block in range(2):
                digit = (x_hi + block) % 2
                columns = slice(block * LANES, block * LANES + LANES)
                high, low = halves(b_v[1, node, y_hi, digit])
                l1[node, 0:128, columns] = high
                l1[node, 256:384, columns] = low

    def receive_1():
        for node in range(2):
            exchange_w1(node).wait_recv()
            for block in range(2):
                digit = (x_hi + block) % 2
                columns = slice(block * LANES, block * LANES + LANES)
                high, low = halves(w1[node, digit])
                l1[node, 128:256, columns] = high
                l1[node, 384:512, columns] = low

    def prepare_2():
        load_b(2).wait()
        for node in range(2):
            for block in range(4):
                high, low = halves(
                    b_v[2, node, (z_lo + block // 2) % 2, (core + block) % 2]
                )
                columns = slice(block * LANES, block * LANES + LANES)
                l2[node, 0:128, columns] = high
                l2[node, 128:256, columns] = low

    def prepare_3():
        load_b(3).wait()
        for node in range(2):
            exchange_w3(node).wait_recv()
            for block in range(2):
                digit = (y_lo + block) % 2
                columns = slice(block * LANES, block * LANES + LANES)
                high, low = halves(b_v[3, node, digit, z_hi])
                l3[node, 0:128, columns] = high
                l3[node, 256:384, columns] = low
                high, low = halves(w3[node, digit])
                l3[node, 128:256, columns] = high
                l3[node, 384:512, columns] = low

    def prepare_e():
        load_e.wait()
        for node in range(2):
            high, low = halves(e_v[node])
            e_w[node, :, 0:LANES] = high
            e_w[node, :, LANES : 2 * LANES] = low

    def level_0(panel):
        first = 2 * panel
        exchange(X1, first).wait_recv()
        exchange(X1, first + 1).wait_recv()
        value = jnp.concatenate([xb[first], xb[first + 1], xr[first], xr[first + 1]], 0)
        both = product(l0[...], value)
        yb[first] = both[:LANES]
        yb[first + 1] = both[LANES:]
        exchange(X2, first).start()
        exchange(X2, first + 1).start()

    def level_1(sub):
        exchange(X2, sub).wait_recv()
        both = product(l1[sub % 2], jnp.concatenate([yb[sub], yr[sub]], 0))
        zs[sub] = both[LANES:]
        exchange(Y2, sub).start()
        zo[sub] = both[:LANES]

    def sum_1(sub):
        exchange(Y2, sub).wait_recv()
        cb[sub] = zo[sub] + zr[sub]
        exchange(Z1, sub).start()
        exchange(CO, sub).start()

    def forward(sub):
        exchange(Z1, sub).wait_recv()
        exchange(FW, sub).start()

    def level_2(sub):
        exchange(CO, sub).wait_recv()
        exchange(FW, sub).wait_recv()
        value = jnp.concatenate([cb[sub], cor[sub], czr[sub], cfr[sub]], 0)
        db[sub] = product(l2[sub % 2], value)
        exchange(Y1, sub).start()

    def level_3(sub):
        exchange(Y1, sub).wait_recv()
        both = product(l3[sub % 2], jnp.concatenate([db[sub], dr[sub]], 0))
        fs[sub] = both[LANES:]
        exchange(Z2, sub).start()
        fo[sub] = both[:LANES]

    def sum_3(sub):
        exchange(Z2, sub).wait_recv()
        high, low = halves(fo[sub] + fr[sub])
        pair = jnp.concatenate([high, low], 1)
        both = dot(e_w[sub % 2], jnp.concatenate([pair, pair], 0))
        columns = pl.ds(pl.multiple_of(sub // 2 * LANES, LANES), LANES)
        out[sub % 2, :, columns] = out[sub % 2, :, columns] + both[:, :LANES] + both[:, LANES:]

    def near_tile(part):
        tile = part // 2

        @pl.when(part % 2 == 0)
        def _():
            load_n(tile).wait()

        node, row = tile // 4, pl.multiple_of(tile % 4 * 256, 256)
        columns = pl.ds(pl.multiple_of(part % 2 * 256, 256), 256)
        high, low = halves(n_v[tile])
        right = s_hi[node, :, columns]
        out[node, pl.ds(row, 256), columns] = (
            dot(high, right) + dot(low, right) + dot(high, s_lo[node, :, columns])
        )

    def when_sub(step, start, body):
        sub = step - start

        @pl.when((sub >= 0) & (sub < SUBS))
        def _():
            body(sub)

    def iteration(step, _):
        when_sub(step, AT_L3, level_3)
        when_sub(step, AT_L2, level_2)
        when_sub(step, AT_FWD, forward)
        when_sub(step, AT_SUM1, sum_1)
        pl.when(step == AT_L1)(receive_1)
        when_sub(step, AT_L1, level_1)

        odd = step - AT_L0 - 1

        @pl.when((odd >= 0) & (odd < SUBS) & (odd % 2 == 0))
        def _():
            level_0(odd // 2)
        when_sub(step, AT_SUM3, sum_3)

        sub = step - AT_SEND

        @pl.when((sub >= ahead) & (sub < SUBS))
        def _():
            exchange(X1, sub).start()

        part = step - NEAR_AT

        @pl.when((part >= 0) & (part < TILES - 2))
        def _():
            load_n(part + 2).start()

        @pl.when(part == TILES - 2)
        def _():
            load_e.start()

        @pl.when((part >= 0) & (part < 2 * TILES))
        def _():
            near_tile(part)

        pl.when(step == 0)(prepare_1)
        pl.when(step == 5)(prepare_2)
        pl.when(step == 7)(prepare_3)
        pl.when(step == AT_SUM3 - 1)(prepare_e)
        return 0

    lax.fori_loop(0, AT_SUM3 + SUBS, iteration, 0)

    def drain(sub, _):
        for step in range(8):
            exchange(step, sub).wait_send()
        return 0

    lax.fori_loop(0, SUBS, drain, 0)
    for node in range(2):
        exchange_w1(node).wait_send()
        exchange_w3(node).wait_send()


def body(sources, near_field, project_factor, expand_factor, butterfly):
    nodes, leaf, _ = near_field.shape
    rhs = sources.shape[1]
    rank = project_factor.shape[1]
    f32, bf16 = jnp.float32, jnp.bfloat16
    block = pltpu.VMEM((SUBS, rank, LANES), f32)
    dma = pltpu.SemaphoreType.DMA
    result = pl.pallas_call(
        kernel,
        out_shape=pltpu.VMEM((nodes, leaf, rhs), f32),
        in_specs=[pl.BlockSpec(memory_space=pl.ANY)] * 5,
        out_specs=pl.BlockSpec(memory_space=pltpu.VMEM),
        scratch_shapes=[
            pltpu.VMEM((4, nodes, leaf, LANES), f32),
            pltpu.VMEM((TILES, 256, leaf), f32),
            pltpu.VMEM((nodes, leaf, rank), f32),
            pltpu.VMEM((nodes, leaf, rank), f32),
            pltpu.VMEM((4, nodes, 2, 2, rank, rank), f32),
            pltpu.VMEM((nodes, leaf, rhs), bf16),
            pltpu.VMEM((nodes, leaf, rhs), bf16),
            pltpu.VMEM((nodes, 2 * rank, leaf), bf16),
            pltpu.VMEM((nodes, leaf, 2 * rank), bf16),
            pltpu.VMEM((4 * rank, 4 * rank), bf16),
            pltpu.VMEM((nodes, 4 * rank, 2 * rank), bf16),
            pltpu.VMEM((nodes, 2 * rank, 4 * rank), bf16),
            pltpu.VMEM((nodes, 4 * rank, 2 * rank), bf16),
            pltpu.VMEM((nodes, 2, rank, rank), f32),
            pltpu.VMEM((nodes, 2, rank, rank), f32),
        ]
        + [block] * 16
        + [
            dma((4,)), dma((TILES,)), dma((2,)), dma((1,)), dma((4,)),
            dma((4,)), dma((4,)), dma((8, SUBS)), dma((8, SUBS)),
        ],
        compiler_params=pltpu.CompilerParams(
            collective_id=0, has_side_effects=True, vmem_limit_bytes=50 * 1024 * 1024
        ),
        name="butterfly",
    )(
        sources.reshape(nodes, leaf, rhs),
        near_field.reshape(TILES, 256, leaf),
        project_factor.reshape(nodes, leaf, rank),
        expand_factor.reshape(nodes, leaf, rank),
        butterfly.reshape(butterfly.shape[0], nodes, 2, 2, rank, rank),
    )
    return result.reshape(nodes * leaf, rhs)


def solution(mesh):
    in_specs = (
        P(("outer", "inner"), None),
        P(("outer", "inner"), None, None),
        P(("outer", "inner"), None),
        P(("outer", "inner"), None),
        P(None, ("outer", "inner"), None, None, None),
    )
    out_specs = P(("outer", "inner"), None)
    return jax.shard_map(body, mesh=mesh, in_specs=in_specs, out_specs=out_specs, check_vma=False)
```
